256 devices in a mesh: gz: 16 (over z, y_lo), pa: 16 (over y_hi, x, core).
Axes of the slice: x: 4, y: 4 (y_hi: 2, y_lo: 2; y = y_hi * 2 + y_lo), z: 8, core: 2. Of those that a mesh axis runs over, the one named last changes fastest.
Arguments:
- density: bfloat16 [64, 1024, 1024], P('gz', 'pa'), may hold values from -6 to 6
- green: float32 [128, 1024, 1024], P('gz', 'pa'), may hold values from 0.1 to 3
Outputs:
- potential: float32 [64, 1024, 1024], P('gz', 'pa')
The draws below stay inside these ranges and needn't reach their ends.
All inputs are finite; a program needn't handle non-finite values.
Results may differ from the reference program's by a relative error of at most 0.02.
Values may be sent and summed in bfloat16 or wider, within the bound.
No kernel may reach another device: no remote copies, remote signals or barrier semaphores. Data moves between devices by JAX's collectives and lax.ppermute only.
A program may use at most 64 MiB of HBM per device.

```python
import math
import jax
import jax.numpy as jnp
from jax import lax

NX = 1024
NY = 1024
NZ = 64
M = 128
N_GZ = 16


def level_of(key, dims, cuts, least, high):
    level = 1.0
    for axis_at, shards_of in cuts:
        steps = jax.random.uniform(jax.random.fold_in(jax.random.fold_in(key, 6), axis_at), (shards_of,), jnp.float32, least / len(cuts), high / len(cuts))
        level = level * jnp.repeat(jnp.exp(steps), dims[axis_at] // shards_of).reshape((-1,) + (1,) * (len(dims) - 1 - axis_at))
    return level


def scatter_about(stream_key, extent, deviation, limit, cuts=(), kind=jnp.bfloat16):
    drawn = jax.random.normal(stream_key, extent, jnp.float32) * deviation
    if len(cuts) > 0:
        drawn = level_of(stream_key, extent, cuts, -0.22, 0.18) * drawn
    return jnp.clip(drawn, min=-limit, max=limit).astype(kind)


def setup_inputs(seed: int = 0) -> dict:
    arg_keys = jax.random.split(jax.random.key(seed), 3)
    return {
        "density": scatter_about(arg_keys[0], (NZ, NX, NY), 1.0, 6.0, ((0, 16), (1, 16))),
        "green": jnp.clip(jnp.exp(math.log(3.0) - 3.4011974 * jax.random.uniform(arg_keys[1], (M, NY, NX), jnp.float32) ** level_of(arg_keys[1], (M, NY, NX), ((0, 16), (1, 16)), -0.2, 0.2)), 0.1, 3.0),
    }


def cas_table(rows, cols, length):
    product = (rows[:, None] * cols[None, :]) % length
    angle = product.astype(jnp.float32) * (2.0 * math.pi / length)
    return (jnp.cos(angle) + jnp.sin(angle)).astype(jnp.bfloat16)


def blocked_sum(tables, pieces, rows, columns):
    def add_block(total, pair):
        table, piece = pair
        term = jnp.dot(table, piece, precision=lax.Precision.HIGHEST, preferred_element_type=jnp.float32).astype(jnp.bfloat16)
        term = lax.optimization_barrier(term)
        return total + term.astype(jnp.float32), None

    total, _ = lax.scan(add_block, jnp.zeros((rows, columns), jnp.float32), (tables, pieces))
    return total


def reference(density, green):
    z_cells, x_cells, y_cells = density.shape
    z_freqs = 2 * z_cells
    z_slab = z_cells // N_GZ
    k_block = z_freqs // N_GZ
    columns = x_cells * y_cells
    highest = lax.Precision.HIGHEST
    f_index = jnp.arange(z_freqs, dtype=jnp.int32)
    z_index = jnp.arange(z_cells, dtype=jnp.int32)
    forward_tables = cas_table(f_index, z_index, z_freqs).astype(jnp.float32).reshape(z_freqs, N_GZ, z_slab).transpose(1, 0, 2)
    slabs = density.astype(jnp.float32).reshape(N_GZ, z_slab, columns)
    zspec = blocked_sum(forward_tables, slabs, z_freqs, columns).astype(jnp.bfloat16).reshape(z_freqs, x_cells, y_cells)
    cas_y = cas_table(jnp.arange(y_cells, dtype=jnp.int32), jnp.arange(y_cells, dtype=jnp.int32), y_cells).astype(jnp.float32)
    cas_x = cas_table(jnp.arange(x_cells, dtype=jnp.int32), jnp.arange(x_cells, dtype=jnp.int32), x_cells).astype(jnp.float32)
    yspec = jnp.einsum('kxy,vy->kxv', zspec.astype(jnp.float32), cas_y, precision=highest).astype(jnp.bfloat16)
    xspec = jnp.einsum('kxv,ux->kvu', yspec.astype(jnp.float32), cas_x, precision=highest)
    weighted = (green * xspec).astype(jnp.bfloat16)
    yback = jnp.einsum('kvu,xu->kxv', weighted.astype(jnp.float32), cas_x, precision=highest).astype(jnp.bfloat16)
    zback = jnp.einsum('kxv,yv->kxy', yback.astype(jnp.float32), cas_y, precision=highest).astype(jnp.bfloat16)
    back_tables = cas_table(z_index, f_index, z_freqs).astype(jnp.float32).reshape(z_cells, N_GZ, k_block).transpose(1, 0, 2)
    blocks = zback.astype(jnp.float32).reshape(N_GZ, k_block, columns)
    total = blocked_sum(back_tables, blocks, z_cells, columns)
    scale = 1.0 / (x_cells * y_cells * z_freqs)
    return (total * scale).reshape(z_cells, x_cells, y_cells)
```

```python
import math

import jax
import jax.numpy as jnp
from jax import lax
from jax.experimental import pallas as pl
from jax.experimental.pallas import tpu as pltpu
from jax.sharding import PartitionSpec as P


F32, BF16 = jnp.float32, jnp.bfloat16
LANES = 128
VMEM = pl.BlockSpec(memory_space=pltpu.VMEM)
SMEM = pl.BlockSpec(memory_space=pltpu.SMEM)
ANY = pl.BlockSpec(memory_space=pl.ANY)


def call(kernel, outs, *args, specs=None, inside=(), keep=False, limit=24, **kwargs):
    args = [pltpu.with_memory_space_constraint(a, pltpu.VMEM) if i in inside else a for i, a in enumerate(args)]
    out_specs = jax.tree.map(lambda _: VMEM, outs)
    if keep:
        outs = jax.tree.map(lambda o: pltpu.VMEM(o.shape, o.dtype), outs)
    return pl.pallas_call(
        kernel,
        out_shape=outs,
        in_specs=specs or [VMEM] * len(args),
        out_specs=out_specs,
        compiler_params=pltpu.CompilerParams(vmem_limit_bytes=limit * 2**20),
        **kwargs,
    )(*args)


def fetch(table_ref, buffer, sem):
    copy = pltpu.make_async_copy(table_ref, buffer, sem)
    copy.start()
    return copy


def array(*shape, dtype=BF16):
    return jax.ShapeDtypeStruct(shape, dtype)


def trig(product, length):
    angle = (product % length).astype(F32) * (2.0 * math.pi / length)
    return jnp.cos(angle), jnp.sin(angle)


def cas_square(length, fine=32):
    k = jnp.arange(length, dtype=jnp.int32)[None, :]
    ca, sa = trig(jnp.arange(length // fine, dtype=jnp.int32)[:, None] * fine * k, length)
    cb, sb = trig(jnp.arange(fine, dtype=jnp.int32)[:, None] * k, length)
    ca, sa, plus, minus = lax.optimization_barrier((ca, sa, cb + sb, cb - sb))
    table = ca[:, None, :] * plus[None] + sa[:, None, :] * minus[None]
    return lax.optimization_barrier(table.reshape(length, length).astype(BF16))


def swap_halves(first, second, axis):
    half = first.shape[axis] // 2
    lower = lax.broadcasted_iota(jnp.int32, first.shape, axis) < half
    return (
        jnp.where(lower, first, pltpu.roll(second, half, axis)),
        jnp.where(lower, pltpu.roll(first, half, axis), second),
    )


def convert_kernel(me_ref, green_ref, *refs):
    *out_refs, buffer, sems = refs
    copies = []
    for s in range(len(out_refs)):
        at = pl.multiple_of(jnp.bitwise_xor(me_ref[0] // 2, s) * 8, 8)
        copies.append(pltpu.make_async_copy(green_ref.at[:, pl.ds(at, 8), :], buffer.at[s], sems.at[s]))
        copies[-1].start()
    for s, out_ref in enumerate(out_refs):
        copies[s].wait()
        out_ref[...] = buffer[s].reshape(out_ref.shape).astype(BF16)


def share_kernel(me_ref, *refs):
    *in_refs, keep_ref, send_ref = refs
    flip = me_ref[0] % 2
    shape = keep_ref.shape[1:]
    for s, in_ref in enumerate(in_refs):
        block = in_ref[...].astype(F32).reshape(in_ref.shape[0] // 16, 2, 8, in_ref.shape[1])
        low, high = swap_halves(block[:, 0], block[:, 1], 1)
        keep_ref[s] = jnp.where(flip == 0, low, high).reshape(shape).astype(BF16)
        send_ref[s] = jnp.where(flip == 0, high, low).reshape(shape).astype(BF16)


def expand_kernel(table_ref, forth_ref, back_ref, *, v_sub):
    small = table_ref[...]
    freqs, cells = small.shape
    rows, cols = forth_ref.shape
    half = cols // 2

    def iota(shape, axis):
        return lax.broadcasted_iota(jnp.int32, shape, axis)

    def z_of(c):
        return c % half // 8 * 4 + c // v_sub % 2 * 2 + c // half

    def ones(mask):
        return jnp.where(mask, 1.0, 0.0).astype(BF16)

    spread = ones(iota((rows, freqs), 0) // v_sub == iota((rows, freqs), 1))
    pick = ones(iota((cells, cols), 0) == z_of(iota((cells, cols), 1)))
    full = jnp.dot(jnp.dot(spread, small, preferred_element_type=F32).astype(BF16), pick, preferred_element_type=F32)
    same = iota((rows, cols), 0) % v_sub == iota((rows, cols), 1) % v_sub
    forth_ref[...] = jnp.where(same, full, 0.0).astype(BF16)
    pick = ones(z_of(iota((cols, cells), 0)) == iota((cols, cells), 1))
    spread = ones(iota((freqs, rows), 1) // v_sub == iota((freqs, rows), 0))
    part = lax.dot_general(pick, small, (((1,), (1,)), ((), ())), preferred_element_type=F32).astype(BF16)
    full = jnp.dot(part, spread, preferred_element_type=F32)
    same = iota((cols, rows), 0) % v_sub == iota((cols, rows), 1) % v_sub
    back_ref[...] = jnp.where(same, full, 0.0).astype(BF16)


def forward_kernel(density_ref, table_ref, out_ref):
    spec = lax.dot_general(table_ref[...], density_ref[...], (((1,), (1,)), ((), ())), preferred_element_type=F32)
    tiles = spec.shape[0] // 8
    left = spec[:, :LANES].reshape(tiles, 8, LANES)
    right = spec[:, LANES:].reshape(tiles, 8, LANES)
    even, odd = swap_halves(left, right, 1)
    out_ref[:, 0] = even.astype(BF16)
    out_ref[:, 1] = odd.astype(BF16)


def spectrum_kernel(moved_ref, table_ref, out_ref, buffer, sem):
    copy = fetch(table_ref, buffer, sem)
    pencils, groups = moved_ref.shape[:2]
    rows = groups * 8
    low, high = [], []
    for q in range(pencils // 2):
        left = moved_ref[2 * q].reshape(rows, LANES).astype(F32)
        right = moved_ref[2 * q + 1].reshape(rows, LANES).astype(F32)
        a, b = swap_halves(left, right, 1)
        low.append(a.astype(BF16))
        high.append(b.astype(BF16))
    data = jnp.concatenate([jnp.concatenate(low, axis=1), jnp.concatenate(high, axis=1)], axis=0)
    copy.wait()
    out_ref[...] = jnp.dot(data, buffer[...], preferred_element_type=F32).astype(BF16)


def solve_kernel(spec_ref, forth_ref, back_ref, table_ref, keep_ref, came_ref, out_ref, buffer, sem):
    copy = fetch(table_ref, buffer, sem)
    zspec = jnp.dot(forth_ref[...], spec_ref[...], preferred_element_type=F32)
    rows = zspec.shape[0] // 2
    shape = (rows, zspec.shape[1])
    weighted = jnp.concatenate(
        [
            (zspec[:rows] * keep_ref[...].reshape(shape).astype(F32)).astype(BF16),
            (zspec[rows:] * came_ref[...].reshape(shape).astype(F32)).astype(BF16),
        ],
        axis=0,
    )
    total = jnp.dot(back_ref[...], weighted, preferred_element_type=F32).astype(BF16)
    copy.wait()
    values = jnp.dot(total, buffer[...], preferred_element_type=F32)
    half = values.shape[0] // 2
    shape = out_ref.shape[1:]
    for q in range(out_ref.shape[0] // 2):
        at = slice(q * LANES, (q + 1) * LANES)
        a, b = swap_halves(values[:half, at], values[half:, at], 1)
        out_ref[2 * q] = a.astype(BF16).reshape(shape)
        out_ref[2 * q + 1] = b.astype(BF16).reshape(shape)


def inverse_kernel(came_ref, table_ref, out_ref, buffer, sem, *, scale):
    copy = fetch(table_ref, buffer, sem)
    even = came_ref[:, 0].astype(F32)
    odd = came_ref[:, 1].astype(F32)
    left, right = swap_halves(even, odd, 1)
    rows = left.shape[0] * 8
    data = jnp.concatenate([left.reshape(rows, LANES), right.reshape(rows, LANES)], axis=1).astype(BF16)
    copy.wait()
    out = lax.dot_general(data, buffer[...], (((0,), (0,)), ((), ())), preferred_element_type=F32)
    out_ref[...] = out * scale


def local(density, green):
    z_slab, x_local, y_cells = density.shape
    k_block, y_local, x_cells = green.shape
    groups = lax.axis_size("gz")
    pencils = lax.axis_size("pa")
    v_sub = y_local // groups
    z_cells = z_slab * groups
    z_freqs = k_block * groups
    lines = z_slab * x_local
    steps = groups // 2
    me = lax.axis_index("gz").astype(jnp.int32)
    place = me.reshape(1)

    pieces = call(
        convert_kernel,
        (array(k_block * 2 * v_sub, x_cells),) * steps,
        place,
        green,
        specs=[SMEM, ANY],
        scratch_shapes=[pltpu.VMEM((steps, k_block, 2 * v_sub, x_cells), F32), pltpu.SemaphoreType.DMA((steps,))],
    )
    pieces = list(pieces)
    for s in range(1, steps):
        pieces[s] = lax.ppermute(pieces[s], "gz", [(i, i ^ 2 * s) for i in range(groups)])
    shape = array(steps, k_block * v_sub, x_cells)
    keep, send = call(share_kernel, (shape, shape), place, *pieces, specs=[SMEM] + [VMEM] * steps)
    came = lax.ppermute(send, "gz", [(i, i ^ 1) for i in range(groups)])

    table = cas_square(y_cells)
    forward = call(forward_kernel, array(y_cells // 8, 2, 8, LANES), density.reshape(lines, y_cells), table, keep=True)
    buffers = [pltpu.VMEM(table.shape, BF16), pltpu.SemaphoreType.DMA]
    moved = lax.all_to_all(
        forward.reshape(pencils * groups, 8, LANES), ("pa", "gz"), split_axis=0, concat_axis=0, tiled=True
    )
    spectrum = call(
        spectrum_kernel,
        array(groups * 16, x_cells),
        moved.reshape(pencils, groups, 8, LANES),
        table,
        inside=(0,),
        specs=[VMEM, ANY],
        scratch_shapes=buffers,
    )

    turn = jnp.arange(steps, dtype=jnp.int32) * 2
    block = jnp.bitwise_xor(me, jnp.concatenate([turn, turn + 1]))
    k_index = (block[:, None] * k_block + jnp.arange(k_block, dtype=jnp.int32)[None, :]).reshape(-1)
    cos, sin = trig(k_index[:, None] * jnp.arange(z_cells, dtype=jnp.int32)[None, :], z_freqs)
    forth, inverse_z = call(
        lambda *refs: expand_kernel(*refs, v_sub=v_sub),
        (array(z_freqs * v_sub, groups * 16), array(groups * 16, z_freqs * v_sub)),
        (cos + sin).astype(BF16),
    )
    solved = call(
        solve_kernel,
        array(pencils, groups, 8, LANES),
        spectrum,
        forth,
        inverse_z,
        table,
        keep,
        came,
        specs=[VMEM, VMEM, VMEM, ANY, VMEM, VMEM],
        keep=True,
        scratch_shapes=buffers,
    )
    back = lax.all_to_all(
        solved.reshape(pencils * groups, 8, LANES), ("pa", "gz"), split_axis=0, concat_axis=0, tiled=True
    )
    scale = 1.0 / (x_cells * y_cells * z_freqs)
    out = call(
        lambda *refs: inverse_kernel(*refs, scale=scale),
        array(lines, y_cells, dtype=F32),
        back.reshape(y_cells // 8, 2, 8, LANES),
        table,
        inside=(0,),
        specs=[VMEM, ANY],
        scratch_shapes=buffers,
    )
    return out.reshape(z_slab, x_local, y_cells)


def solution(mesh):
    return jax.shard_map(
        local,
        mesh=mesh,
        in_specs=(P("gz", "pa", None), P("gz", "pa", None)),
        out_specs=P("gz", "pa", None),
        check_vma=False,
    )
```

```python
import math

import jax
import jax.numpy as jnp
from jax import lax
from jax.experimental import pallas as pl
from jax.experimental.pallas import tpu as pltpu
from jax.sharding import PartitionSpec as P


F32, BF16, I32 = jnp.float32, jnp.bfloat16, jnp.int32
LANES = 128
VMEM = pl.BlockSpec(memory_space=pltpu.VMEM)
SMEM = pl.BlockSpec(memory_space=pltpu.SMEM)
ANY = pl.BlockSpec(memory_space=pl.ANY)


def call(kernel, outs, *args, specs=None, keep=True, limit=24, **kwargs):
    specs = specs or [VMEM] * len(args)
    placed = []
    for a, s in zip(args, specs):
        placed.append(a if s is SMEM else pltpu.with_memory_space_constraint(a, pltpu.HBM if s is ANY else pltpu.VMEM))
    out_specs = jax.tree.map(lambda _: VMEM, outs)
    if keep:
        outs = jax.tree.map(lambda o: pltpu.VMEM(o.shape, o.dtype), outs)
    return pl.pallas_call(
        kernel,
        out_shape=outs,
        in_specs=specs,
        out_specs=out_specs,
        compiler_params=pltpu.CompilerParams(vmem_limit_bytes=limit * 2**20),
        **kwargs,
    )(*placed)


def array(*shape, dtype=BF16):
    return jax.ShapeDtypeStruct(shape, dtype)


def iota(shape, axis):
    return lax.broadcasted_iota(I32, shape, axis)


def trig(product, length):
    angle = lax.rem(product, jnp.full_like(product, length)).astype(F32) * (2.0 * math.pi / length)
    return jnp.cos(angle), jnp.sin(angle)


def cas_square(table_ref):
    length = table_ref.shape[0]
    coarse = length // 64
    k = iota((8, length), 1)
    cc, sc = trig(iota((8, length), 0) * k, length)
    cb, sb = trig(iota((8, length), 0) * 8 * k, length)
    high = [trig((iota((8, length), 0) + 8 * i) * 64 * k, length) for i in range(coarse // 8)]
    cbc = [cb[b : b + 1] * cc - sb[b : b + 1] * sc for b in range(8)]
    sbc = [sb[b : b + 1] * cc + cb[b : b + 1] * sc for b in range(8)]
    cbc, sbc = jnp.concatenate(cbc, axis=0), jnp.concatenate(sbc, axis=0)
    plus, minus = cbc + sbc, cbc - sbc
    for a in range(coarse):
        ca, sa = (x[a % 8 : a % 8 + 1] for x in high[a // 8])
        table_ref[64 * a : 64 * (a + 1)] = (ca * plus + sa * minus).astype(BF16)


def swap_halves(first, second, axis):
    half = first.shape[axis] // 2
    lower = iota(first.shape, axis) < half
    return (
        jnp.where(lower, first, pltpu.roll(second, half, axis)),
        jnp.where(lower, pltpu.roll(first, half, axis), second),
    )


def share(block, flip, keep_ref, send_ref, at):
    shape = keep_ref.shape[1:]
    block = block.reshape(block.shape[0] // 16, 2, 8, block.shape[1])
    low, high = swap_halves(block[:, 0], block[:, 1], 1)
    keep_ref[at] = jnp.where(flip == 0, low, high).reshape(shape).astype(BF16)
    send_ref[at] = jnp.where(flip == 0, high, low).reshape(shape).astype(BF16)


def split_kernel(me_ref, green_ref, keep_ref, send_ref, *refs, near, far, steps):
    *far_refs, buffer, sems = refs
    copies = []
    for i, s in enumerate(near + far):
        at = pl.multiple_of(along_z(me_ref[0] // 2, s, steps) * 8, 8)
        copies.append(pltpu.make_async_copy(green_ref.at[:, pl.ds(at, 8), :], buffer.at[i], sems.at[i]))
        copies[-1].start()
    for i in range(len(near + far)):
        copies[i].wait()
        block = buffer[i]
        block = block.reshape(block.shape[0] * block.shape[1], block.shape[2])
        if i < len(near):
            share(block, me_ref[0] % 2, keep_ref, send_ref, i)
        else:
            far_refs[i - len(near)][...] = block.astype(BF16)


def share_kernel(me_ref, *refs):
    *in_refs, keep_ref, send_ref = refs
    for i, in_ref in enumerate(in_refs):
        share(in_ref[...].astype(F32), me_ref[0] % 2, keep_ref, send_ref, i)


def join_kernel(keep_ref, came_ref, *out_refs):
    rows = keep_ref.shape[1]
    for i, out_ref in enumerate(out_refs):
        out_ref[:rows] = keep_ref[i + 1]
        out_ref[rows:] = came_ref[i + 1]


def expand_kernel(me_ref, forth_ref, back_ref, *, order, groups, v_sub, k_block, z_slab):
    rows, cols = forth_ref.shape
    half, steps = cols // 2, groups // 2
    freqs, cells = groups * k_block, groups * z_slab
    r = iota((freqs, cells), 0)
    step, turn = jnp.zeros_like(r), jnp.zeros_like(r)
    for i, (s, sy) in enumerate(order):
        step = jnp.where(r // k_block == i, s, step)
        turn = jnp.where(r // k_block == i, sy, turn)
    from_z = along_z(me_ref[0] // 2, step, steps, sign=-1)
    from_y = jnp.bitwise_xor(me_ref[0] % 2, turn)
    cos, sin = trig(((from_z * 2 + from_y) * k_block + r % k_block) * iota((freqs, cells), 1), freqs)
    small = (cos + sin).astype(BF16)

    def z_of(c):
        return c % half // 8 * z_slab + c // v_sub % 2 * 2 + c // half

    def ones(mask):
        return jnp.where(mask, 1.0, 0.0).astype(BF16)

    spread = ones(iota((rows, freqs), 0) // v_sub == iota((rows, freqs), 1))
    pick = ones(iota((cells, cols), 0) == z_of(iota((cells, cols), 1)))
    full = jnp.dot(jnp.dot(spread, small, preferred_element_type=F32).astype(BF16), pick, preferred_element_type=F32)
    same = iota((rows, cols), 0) % v_sub == iota((rows, cols), 1) % v_sub
    forth_ref[...] = jnp.where(same, full, 0.0).astype(BF16)
    pick = ones(z_of(iota((cols, cells), 0)) == iota((cols, cells), 1))
    spread = ones(iota((freqs, rows), 1) // v_sub == iota((freqs, rows), 0))
    part = lax.dot_general(pick, small, (((1,), (1,)), ((), ())), preferred_element_type=F32).astype(BF16)
    full = jnp.dot(part, spread, preferred_element_type=F32)
    same = iota((cols, rows), 0) % v_sub == iota((cols, rows), 1) % v_sub
    back_ref[...] = jnp.where(same, full, 0.0).astype(BF16)


def forward_kernel(density_ref, out_ref, table_ref):
    cas_square(table_ref)
    spec = lax.dot_general(table_ref[...], density_ref[...], (((1,), (1,)), ((), ())), preferred_element_type=F32)
    tiles = spec.shape[0] // 8
    left = spec[:, :LANES].reshape(tiles, 8, LANES)
    right = spec[:, LANES:].reshape(tiles, 8, LANES)
    even, odd = swap_halves(left, right, 1)
    out_ref[:, 0] = even.astype(BF16)
    out_ref[:, 1] = odd.astype(BF16)


def spectrum_kernel(moved_ref, table_ref, out_ref):
    pencils, groups = moved_ref.shape[:2]
    rows = groups * 8
    low, high = [], []
    for q in range(pencils // 2):
        left = moved_ref[2 * q].reshape(rows, LANES).astype(F32)
        right = moved_ref[2 * q + 1].reshape(rows, LANES).astype(F32)
        a, b = swap_halves(left, right, 1)
        low.append(a.astype(BF16))
        high.append(b.astype(BF16))
    data = jnp.concatenate([jnp.concatenate(low, axis=1), jnp.concatenate(high, axis=1)], axis=0)
    out_ref[...] = jnp.dot(data, table_ref[...], preferred_element_type=F32).astype(BF16)


def solve_kernel(spec_ref, forth_ref, back_ref, table_ref, *refs):
    *near_refs, keep_near_ref, keep_far_ref, came_near_ref, came_far_ref, out_ref = refs
    zspec = jnp.dot(forth_ref[...], spec_ref[...], preferred_element_type=F32)
    blocks = [ref[...] for ref in near_refs]
    for near_ref, far_ref in ((keep_near_ref, keep_far_ref), (came_near_ref, came_far_ref)):
        blocks.append(near_ref[0])
        blocks.extend(far_ref[i] for i in range(far_ref.shape[0]))
    parts, at = [], 0
    for block in blocks:
        parts.append((zspec[at : at + block.shape[0]] * block.astype(F32)).astype(BF16))
        at += block.shape[0]
    weighted = jnp.concatenate(parts, axis=0)
    total = jnp.dot(back_ref[...], weighted, preferred_element_type=F32).astype(BF16)
    values = jnp.dot(total, table_ref[...], preferred_element_type=F32)
    half = values.shape[0] // 2
    shape = out_ref.shape[1:]
    for q in range(out_ref.shape[0] // 2):
        at = slice(q * LANES, (q + 1) * LANES)
        a, b = swap_halves(values[:half, at], values[half:, at], 1)
        out_ref[2 * q] = a.astype(BF16).reshape(shape)
        out_ref[2 * q + 1] = b.astype(BF16).reshape(shape)


def inverse_kernel(came_ref, table_ref, out_ref, *, scale):
    left, right = swap_halves(came_ref[:, 0].astype(F32), came_ref[:, 1].astype(F32), 1)
    rows = left.shape[0] * 8
    data = jnp.concatenate([left.reshape(rows, LANES), right.reshape(rows, LANES)], axis=1).astype(BF16)
    out = lax.dot_general(data, table_ref[...], (((0,), (0,)), ((), ())), preferred_element_type=F32)
    out_ref[...] = out * scale


def along_z(z, s, steps, sign=1):
    return (z + sign * s) & (steps - 1)


def local(density, green):
    z_slab, x_local, y_cells = density.shape
    k_block, y_local, x_cells = green.shape
    groups = lax.axis_size("gz")
    pencils = lax.axis_size("pa")
    v_sub = y_local // groups
    z_freqs = k_block * groups
    lines = z_slab * x_local
    steps = groups // 2
    place = lax.axis_index("gz").astype(I32).reshape(1)

    near, far = (0, 1, steps - 1, 2, steps - 2), tuple(range(3, steps - 2))
    order = [(s, sy) for s in near[1:] for sy in (0, 1)] + [(s, sy) for sy in (0, 1) for s in (0, *far)]

    def shift_z(piece, s):
        pairs = [(i, along_z(i // 2, s, steps) * 2 + i % 2) for i in range(groups)]
        return lax.ppermute(piece, "gz", pairs)

    def swap_y(piece):
        return lax.ppermute(piece, "gz", [(i, i ^ 1) for i in range(groups)])

    rows = k_block * v_sub
    shared = array(len(near), rows, x_cells)
    keep_near, send_near, *outward = call(
        lambda *refs: split_kernel(*refs, near=near, far=far, steps=steps),
        (shared, shared) + (array(2 * rows, x_cells),) * len(far),
        place,
        green,
        specs=[SMEM, ANY],
        scratch_shapes=[pltpu.VMEM((steps, k_block, 2 * v_sub, x_cells), F32), pltpu.SemaphoreType.DMA((steps,))],
    )
    came_near = swap_y(send_near)
    inward = [shift_z(piece, s) for piece, s in zip(outward, far)]
    shared = array(len(far), rows, x_cells)
    keep_far, send_far = call(share_kernel, (shared, shared), place, *inward, specs=[SMEM] + [VMEM] * len(far))
    came_far = swap_y(send_far)
    pieces = call(join_kernel, (array(2 * rows, x_cells),) * (len(near) - 1), keep_near, came_near)
    pieces = [shift_z(piece, s) for piece, s in zip(pieces, near[1:])]

    forward, table = call(
        forward_kernel, (array(y_cells // 8, 2, 8, LANES), array(y_cells, y_cells)), density.reshape(lines, y_cells)
    )
    moved = lax.all_to_all(
        forward.reshape(pencils * groups, 8, LANES), ("pa", "gz"), split_axis=0, concat_axis=0, tiled=True
    )
    spectrum = call(spectrum_kernel, array(groups * 16, x_cells), moved.reshape(pencils, groups, 8, LANES), table)
    forth, inverse_z = call(
        lambda *refs: expand_kernel(*refs, order=order, groups=groups, v_sub=v_sub, k_block=k_block, z_slab=z_slab),
        (array(z_freqs * v_sub, groups * 16), array(groups * 16, z_freqs * v_sub)),
        place,
        specs=[SMEM],
    )
    solved = call(
        solve_kernel,
        array(pencils, groups, 8, LANES),
        spectrum,
        forth,
        inverse_z,
        table,
        *pieces,
        keep_near,
        keep_far,
        came_near,
        came_far,
    )
    back = lax.all_to_all(
        solved.reshape(pencils * groups, 8, LANES), ("pa", "gz"), split_axis=0, concat_axis=0, tiled=True
    )
    scale = 1.0 / (x_cells * y_cells * z_freqs)
    out = call(
        lambda *refs: inverse_kernel(*refs, scale=scale),
        array(lines, y_cells, dtype=F32),
        back.reshape(y_cells // 8, 2, 8, LANES),
        table,
        keep=False,
    )
    return out.reshape(z_slab, x_local, y_cells)


def solution(mesh):
    return jax.shard_map(
        local,
        mesh=mesh,
        in_specs=(P("gz", "pa", None), P("gz", "pa", None)),
        out_specs=P("gz", "pa", None),
        check_vma=False,
    )
```

```python
import math

import jax
import jax.numpy as jnp
from jax import lax
from jax.experimental import pallas as pl
from jax.experimental.pallas import tpu as pltpu
from jax.sharding import PartitionSpec as P


F32, BF16, I32 = jnp.float32, jnp.bfloat16, jnp.int32
LANES = 128
VMEM = pl.BlockSpec(memory_space=pltpu.VMEM)
SMEM = pl.BlockSpec(memory_space=pltpu.SMEM)
ANY = pl.BlockSpec(memory_space=pl.ANY)


def call(kernel, outs, *args, specs=None, results=None, limit=24, **kwargs):
    specs = specs or [VMEM] * len(args)
    placed = []
    for a, s in zip(args, specs):
        placed.append(a if s is SMEM else pltpu.with_memory_space_constraint(a, pltpu.HBM if s is ANY else pltpu.VMEM))
    results = results or jax.tree.map(lambda _: VMEM, outs)
    return pl.pallas_call(
        kernel,
        out_shape=outs,
        in_specs=specs,
        out_specs=results,
        compiler_params=pltpu.CompilerParams(vmem_limit_bytes=limit * 2**20),
        **kwargs,
    )(*placed)


def send(buffer, out_ref, sem):
    copy = pltpu.make_async_copy(buffer, out_ref, sem)
    copy.start()
    return copy


def array(*shape, dtype=BF16):
    return jax.ShapeDtypeStruct(shape, dtype)


def iota(shape, axis):
    return lax.broadcasted_iota(I32, shape, axis)


def trig(product, length):
    angle = lax.rem(product, jnp.full_like(product, length)).astype(F32) * (2.0 * math.pi / length)
    return jnp.cos(angle), jnp.sin(angle)


def cas_square(table_ref):
    length = table_ref.shape[0]
    coarse = length // 64
    k = iota((8, length), 1)
    cc, sc = trig(iota((8, length), 0) * k, length)
    cb, sb = trig(iota((8, length), 0) * 8 * k, length)
    high = [trig((iota((8, length), 0) + 8 * i) * 64 * k, length) for i in range(coarse // 8)]
    cbc = [cb[b : b + 1] * cc - sb[b : b + 1] * sc for b in range(8)]
    sbc = [sb[b : b + 1] * cc + cb[b : b + 1] * sc for b in range(8)]
    cbc, sbc = jnp.concatenate(cbc, axis=0), jnp.concatenate(sbc, axis=0)
    plus, minus = cbc + sbc, cbc - sbc
    for a in range(coarse):
        ca, sa = (x[a % 8 : a % 8 + 1] for x in high[a // 8])
        table_ref[64 * a : 64 * (a + 1)] = (ca * plus + sa * minus).astype(BF16)


def swap_halves(first, second, axis):
    half = first.shape[axis] // 2
    lower = iota(first.shape, axis) < half
    return (
        jnp.where(lower, first, pltpu.roll(second, half, axis)),
        jnp.where(lower, pltpu.roll(first, half, axis), second),
    )


def share(block, flip, keep_ref, send_ref, at):
    shape = keep_ref.shape[1:]
    block = block.reshape(block.shape[0] // 16, 2, 8, block.shape[1])
    low, high = swap_halves(block[:, 0], block[:, 1], 1)
    keep_ref[at] = jnp.where(flip == 0, low, high).reshape(shape).astype(BF16)
    send_ref[at] = jnp.where(flip == 0, high, low).reshape(shape).astype(BF16)


def split_kernel(me_ref, green_ref, keep_ref, send_ref, *refs, near, far, steps):
    *far_refs, buffer, near_buffer, far_buffer, sems, out_sems = refs
    copies, sent = [], []
    for i, s in enumerate(far + near):
        at = pl.multiple_of(along_z(me_ref[0] // 2, s, steps) * 8, 8)
        copies.append(pltpu.make_async_copy(green_ref.at[:, pl.ds(at, 8), :], buffer.at[i], sems.at[i]))
        copies[-1].start()
    for i in range(len(far + near)):
        copies[i].wait()
        block = buffer[i]
        block = block.reshape(block.shape[0] * block.shape[1], block.shape[2])
        n = i - len(far)
        if n < 0:
            far_buffer[i] = block.astype(BF16)
            sent.append(send(far_buffer.at[i], far_refs[i], out_sems.at[i]))
        else:
            share(block, me_ref[0] % 2, keep_ref, near_buffer, n)
            sent.append(send(near_buffer.at[n], send_ref.at[n], out_sems.at[i]))
    for copy in sent:
        copy.wait()


def share_kernel(me_ref, *refs):
    *in_refs, keep_ref, send_ref = refs
    for i, in_ref in enumerate(in_refs):
        share(in_ref[...].astype(F32), me_ref[0] % 2, keep_ref, send_ref, i)


def join_kernel(keep_ref, came_ref, *out_refs):
    rows = keep_ref.shape[1]
    for i, out_ref in enumerate(out_refs):
        out_ref[:rows] = keep_ref[i + 1]
        out_ref[rows:] = came_ref[i + 1]


def expand_kernel(me_ref, forth_ref, back_ref, *, order, groups, v_sub, k_block, z_slab):
    rows, cols = forth_ref.shape
    half, steps = cols // 2, groups // 2
    freqs, cells = groups * k_block, groups * z_slab
    r = iota((freqs, cells), 0)
    step, turn = jnp.zeros_like(r), jnp.zeros_like(r)
    for i, (s, sy) in enumerate(order):
        step = jnp.where(r // k_block == i, s, step)
        turn = jnp.where(r // k_block == i, sy, turn)
    from_z = along_z(me_ref[0] // 2, step, steps, sign=-1)
    from_y = jnp.bitwise_xor(me_ref[0] % 2, turn)
    cos, sin = trig(((from_z * 2 + from_y) * k_block + r % k_block) * iota((freqs, cells), 1), freqs)
    small = (cos + sin).astype(BF16)

    def z_of(c):
        return c % half // 8 * z_slab + c // v_sub % 2 * 2 + c // half

    def ones(mask):
        return jnp.where(mask, 1.0, 0.0).astype(BF16)

    spread = ones(iota((rows, freqs), 0) // v_sub == iota((rows, freqs), 1))
    pick = ones(iota((cells, cols), 0) == z_of(iota((cells, cols), 1)))
    full = jnp.dot(jnp.dot(spread, small, preferred_element_type=F32).astype(BF16), pick, preferred_element_type=F32)
    same = iota((rows, cols), 0) % v_sub == iota((rows, cols), 1) % v_sub
    forth_ref[...] = jnp.where(same, full, 0.0).astype(BF16)
    pick = ones(z_of(iota((cols, cells), 0)) == iota((cols, cells), 1))
    spread = ones(iota((freqs, rows), 1) // v_sub == iota((freqs, rows), 0))
    part = lax.dot_general(pick, small, (((1,), (1,)), ((), ())), preferred_element_type=F32).astype(BF16)
    full = jnp.dot(part, spread, preferred_element_type=F32)
    same = iota((cols, rows), 0) % v_sub == iota((cols, rows), 1) % v_sub
    back_ref[...] = jnp.where(same, full, 0.0).astype(BF16)


def forward_kernel(density_ref, out_ref, table_ref):
    cas_square(table_ref)
    spec = lax.dot_general(table_ref[...], density_ref[...], (((1,), (1,)), ((), ())), preferred_element_type=F32)
    tiles = spec.shape[0] // 8
    left = spec[:, :LANES].reshape(tiles, 8, LANES)
    right = spec[:, LANES:].reshape(tiles, 8, LANES)
    even, odd = swap_halves(left, right, 1)
    out_ref[:, 0] = even.astype(BF16)
    out_ref[:, 1] = odd.astype(BF16)


def spectrum_kernel(moved_ref, table_ref, out_ref):
    pencils, groups = moved_ref.shape[:2]
    rows = groups * 8
    low, high = [], []
    for q in range(pencils // 2):
        left = moved_ref[2 * q].reshape(rows, LANES).astype(F32)
        right = moved_ref[2 * q + 1].reshape(rows, LANES).astype(F32)
        a, b = swap_halves(left, right, 1)
        low.append(a.astype(BF16))
        high.append(b.astype(BF16))
    data = jnp.concatenate([jnp.concatenate(low, axis=1), jnp.concatenate(high, axis=1)], axis=0)
    out_ref[...] = jnp.dot(data, table_ref[...], preferred_element_type=F32).astype(BF16)


def solve_kernel(spec_ref, forth_ref, back_ref, table_ref, *refs):
    *near_refs, keep_near_ref, keep_far_ref, came_near_ref, came_far_ref, out_ref = refs
    zspec = jnp.dot(forth_ref[...], spec_ref[...], preferred_element_type=F32)
    blocks = [ref[...] for ref in near_refs]
    for near_ref, far_ref in ((keep_near_ref, keep_far_ref), (came_near_ref, came_far_ref)):
        blocks.append(near_ref[0])
        blocks.extend(far_ref[i] for i in range(far_ref.shape[0]))
    parts, at = [], 0
    for block in blocks:
        parts.append((zspec[at : at + block.shape[0]] * block.astype(F32)).astype(BF16))
        at += block.shape[0]
    weighted = jnp.concatenate(parts, axis=0)
    total = jnp.dot(back_ref[...], weighted, preferred_element_type=F32).astype(BF16)
    values = jnp.dot(total, table_ref[...], preferred_element_type=F32)
    half = values.shape[0] // 2
    shape = out_ref.shape[1:]
    for q in range(out_ref.shape[0] // 2):
        at = slice(q * LANES, (q + 1) * LANES)
        a, b = swap_halves(values[:half, at], values[half:, at], 1)
        out_ref[2 * q] = a.astype(BF16).reshape(shape)
        out_ref[2 * q + 1] = b.astype(BF16).reshape(shape)


def inverse_kernel(came_ref, table_ref, out_ref, buffer, sems, *, scale):
    halves = swap_halves(came_ref[:, 0].astype(F32), came_ref[:, 1].astype(F32), 1)
    sent = []
    for i, half in enumerate(halves):
        data = half.reshape(half.shape[0] * 8, LANES).astype(BF16)
        out = lax.dot_general(data, table_ref[...], (((0,), (0,)), ((), ())), preferred_element_type=F32)
        at = pl.ds(i * LANES, LANES)
        buffer[at] = out * scale
        sent.append(send(buffer.at[at], out_ref.at[at], sems.at[i]))
    for copy in sent:
        copy.wait()


def along_z(z, s, steps, sign=1):
    return (z + sign * s) & (steps - 1)


def local(density, green):
    z_slab, x_local, y_cells = density.shape
    k_block, y_local, x_cells = green.shape
    groups = lax.axis_size("gz")
    pencils = lax.axis_size("pa")
    v_sub = y_local // groups
    z_freqs = k_block * groups
    lines = z_slab * x_local
    steps = groups // 2
    place = lax.axis_index("gz").astype(I32).reshape(1)

    near, far = (0, 1, steps - 1, 2, steps - 2), tuple(range(3, steps - 2))
    order = [(s, sy) for s in near[1:] for sy in (0, 1)] + [(s, sy) for sy in (0, 1) for s in (0, *far)]

    def shift_z(piece, s):
        pairs = [(i, along_z(i // 2, s, steps) * 2 + i % 2) for i in range(groups)]
        return lax.ppermute(piece, "gz", pairs)

    def swap_y(piece):
        return lax.ppermute(piece, "gz", [(i, i ^ 1) for i in range(groups)])

    rows = k_block * v_sub
    shared = array(len(near), rows, x_cells)
    keep_near, send_near, *outward = call(
        lambda *refs: split_kernel(*refs, near=near, far=far, steps=steps),
        (shared, shared) + (array(2 * rows, x_cells),) * len(far),
        place,
        green,
        specs=[SMEM, ANY],
        results=(VMEM, ANY) + (ANY,) * len(far),
        scratch_shapes=[
            pltpu.VMEM((steps, k_block, 2 * v_sub, x_cells), F32),
            pltpu.VMEM(shared.shape, BF16),
            pltpu.VMEM((len(far), 2 * rows, x_cells), BF16),
            pltpu.SemaphoreType.DMA((steps,)),
            pltpu.SemaphoreType.DMA((steps,)),
        ],
    )
    came_near = swap_y(send_near)
    inward = [shift_z(piece, s) for piece, s in zip(outward, far)]
    shared = array(len(far), rows, x_cells)
    keep_far, send_far = call(share_kernel, (shared, shared), place, *inward, specs=[SMEM] + [VMEM] * len(far))
    came_far = swap_y(send_far)
    pieces = call(join_kernel, (array(2 * rows, x_cells),) * (len(near) - 1), keep_near, came_near)
    pieces = [shift_z(piece, s) for piece, s in zip(pieces, near[1:])]

    forward, table = call(
        forward_kernel, (array(y_cells // 8, 2, 8, LANES), array(y_cells, y_cells)), density.reshape(lines, y_cells)
    )
    moved = lax.all_to_all(
        forward.reshape(pencils * groups, 8, LANES), ("pa", "gz"), split_axis=0, concat_axis=0, tiled=True
    )
    spectrum = call(spectrum_kernel, array(groups * 16, x_cells), moved.reshape(pencils, groups, 8, LANES), table)
    forth, inverse_z = call(
        lambda *refs: expand_kernel(*refs, order=order, groups=groups, v_sub=v_sub, k_block=k_block, z_slab=z_slab),
        (array(z_freqs * v_sub, groups * 16), array(groups * 16, z_freqs * v_sub)),
        place,
        specs=[SMEM],
    )
    solved = call(
        solve_kernel,
        array(pencils, groups, 8, LANES),
        spectrum,
        forth,
        inverse_z,
        table,
        *pieces,
        keep_near,
        keep_far,
        came_near,
        came_far,
    )
    back = lax.all_to_all(
        solved.reshape(pencils * groups, 8, LANES), ("pa", "gz"), split_axis=0, concat_axis=0, tiled=True
    )
    scale = 1.0 / (x_cells * y_cells * z_freqs)
    out = call(
        lambda *refs: inverse_kernel(*refs, scale=scale),
        array(lines, y_cells, dtype=F32),
        back.reshape(y_cells // 8, 2, 8, LANES),
        table,
        results=ANY,
        scratch_shapes=[pltpu.VMEM((lines, y_cells), F32), pltpu.SemaphoreType.DMA((lines // LANES,))],
    )
    return out.reshape(z_slab, x_local, y_cells)


def solution(mesh):
    return jax.shard_map(
        local,
        mesh=mesh,
        in_specs=(P("gz", "pa", None), P("gz", "pa", None)),
        out_specs=P("gz", "pa", None),
        check_vma=False,
    )
```

```python
import math

import jax
import jax.numpy as jnp
from jax import lax
from jax.experimental import pallas as pl
from jax.experimental.pallas import tpu as pltpu
from jax.sharding import PartitionSpec as P


F32, BF16, I32 = jnp.float32, jnp.bfloat16, jnp.int32
LANES = 128
VMEM = pl.BlockSpec(memory_space=pltpu.VMEM)
SMEM = pl.BlockSpec(memory_space=pltpu.SMEM)
ANY = pl.BlockSpec(memory_space=pl.ANY)


def call(kernel, outs, *args, specs=None, results=None, limit=24, **kwargs):
    specs = specs or [VMEM] * len(args)
    placed = []
    for a, s in zip(args, specs):
        placed.append(a if s is SMEM else pltpu.with_memory_space_constraint(a, pltpu.HBM if s is ANY else pltpu.VMEM))
    results = results or jax.tree.map(lambda _: VMEM, outs)
    return pl.pallas_call(
        kernel,
        out_shape=outs,
        in_specs=specs,
        out_specs=results,
        compiler_params=pltpu.CompilerParams(vmem_limit_bytes=limit * 2**20),
        **kwargs,
    )(*placed)


def send(buffer, out_ref, sem):
    copy = pltpu.make_async_copy(buffer, out_ref, sem)
    copy.start()
    return copy


def array(*shape, dtype=BF16):
    return jax.ShapeDtypeStruct(shape, dtype)


def iota(shape, axis):
    return lax.broadcasted_iota(I32, shape, axis)


def trig(product, length):
    angle = lax.rem(product, jnp.full_like(product, length)).astype(F32) * (2.0 * math.pi / length)
    return jnp.cos(angle), jnp.sin(angle)


def cas_square(table_ref):
    length = table_ref.shape[0]
    coarse = length // 64
    k = iota((8, length), 1)
    cc, sc = trig(iota((8, length), 0) * k, length)
    cb, sb = trig(iota((8, length), 0) * 8 * k, length)
    high = [trig((iota((8, length), 0) + 8 * i) * 64 * k, length) for i in range(coarse // 8)]
    cbc = [cb[b : b + 1] * cc - sb[b : b + 1] * sc for b in range(8)]
    sbc = [sb[b : b + 1] * cc + cb[b : b + 1] * sc for b in range(8)]
    cbc, sbc = jnp.concatenate(cbc, axis=0), jnp.concatenate(sbc, axis=0)
    plus, minus = cbc + sbc, cbc - sbc
    for a in range(coarse):
        ca, sa = (x[a % 8 : a % 8 + 1] for x in high[a // 8])
        table_ref[64 * a : 64 * (a + 1)] = (ca * plus + sa * minus).astype(BF16)


def swap_halves(first, second, axis):
    half = first.shape[axis] // 2
    lower = iota(first.shape, axis) < half
    return (
        jnp.where(lower, first, pltpu.roll(second, half, axis)),
        jnp.where(lower, pltpu.roll(first, half, axis), second),
    )


def share(block, flip, keep_ref, send_ref, at):
    shape = keep_ref.shape[1:]
    block = block.reshape(block.shape[0] // 16, 2, 8, block.shape[1])
    low, high = swap_halves(block[:, 0], block[:, 1], 1)
    keep_ref[at] = jnp.where(flip == 0, low, high).reshape(shape).astype(BF16)
    send_ref[at] = jnp.where(flip == 0, high, low).reshape(shape).astype(BF16)


def split_kernel(me_ref, green_ref, keep_ref, send_ref, *refs, near, far, steps):
    *far_refs, buffer, near_buffer, far_buffer, sems, out_sems = refs
    copies, sent = [], []
    for i, s in enumerate(far + near):
        at = pl.multiple_of(along_z(me_ref[0] // 2, s, steps) * 8, 8)
        copies.append(pltpu.make_async_copy(green_ref.at[:, pl.ds(at, 8), :], buffer.at[i], sems.at[i]))
        copies[-1].start()
    for i in range(len(far + near)):
        copies[i].wait()
        block = buffer[i]
        block = block.reshape(block.shape[0] * block.shape[1], block.shape[2])
        n = i - len(far)
        if n < 0:
            far_buffer[i] = block.astype(BF16)
            sent.append(send(far_buffer.at[i], far_refs[i], out_sems.at[i]))
        else:
            share(block, me_ref[0] % 2, keep_ref, near_buffer, n)
            sent.append(send(near_buffer.at[n], send_ref.at[n], out_sems.at[i]))
    for copy in sent:
        copy.wait()


def share_kernel(me_ref, *refs):
    *in_refs, keep_ref, send_ref = refs
    for i, in_ref in enumerate(in_refs):
        share(in_ref[...].astype(F32), me_ref[0] % 2, keep_ref, send_ref, i)


def join_kernel(keep_ref, came_ref, *out_refs):
    rows = keep_ref.shape[1]
    for i, out_ref in enumerate(out_refs):
        out_ref[:rows] = keep_ref[i + 1]
        out_ref[rows:] = came_ref[i + 1]


def expand_kernel(me_ref, forth_ref, back_ref, *, order, groups, v_sub, k_block, z_slab):
    rows, cols = forth_ref.shape
    half, steps = cols // 2, groups // 2
    freqs, cells = groups * k_block, groups * z_slab
    r = iota((freqs, cells), 0)
    step, turn = jnp.zeros_like(r), jnp.zeros_like(r)
    for i, (s, sy) in enumerate(order):
        step = jnp.where(r // k_block == i, s, step)
        turn = jnp.where(r // k_block == i, sy, turn)
    from_z = along_z(me_ref[0] // 2, step, steps, sign=-1)
    from_y = jnp.bitwise_xor(me_ref[0] % 2, turn)
    cos, sin = trig(((from_z * 2 + from_y) * k_block + r % k_block) * iota((freqs, cells), 1), freqs)
    small = (cos + sin).astype(BF16)

    def z_of(c):
        return c % half // 8 * z_slab + c // v_sub % 2 * 2 + c // half

    def ones(mask):
        return jnp.where(mask, 1.0, 0.0).astype(BF16)

    spread = ones(iota((rows, freqs), 0) // v_sub == iota((rows, freqs), 1))
    pick = ones(iota((cells, cols), 0) == z_of(iota((cells, cols), 1)))
    full = jnp.dot(jnp.dot(spread, small, preferred_element_type=F32).astype(BF16), pick, preferred_element_type=F32)
    same = iota((rows, cols), 0) % v_sub == iota((rows, cols), 1) % v_sub
    forth_ref[...] = jnp.where(same, full, 0.0).astype(BF16)
    pick = ones(z_of(iota((cols, cells), 0)) == iota((cols, cells), 1))
    spread = ones(iota((freqs, rows), 1) // v_sub == iota((freqs, rows), 0))
    part = lax.dot_general(pick, small, (((1,), (1,)), ((), ())), preferred_element_type=F32).astype(BF16)
    full = jnp.dot(part, spread, preferred_element_type=F32)
    same = iota((cols, rows), 0) % v_sub == iota((cols, rows), 1) % v_sub
    back_ref[...] = jnp.where(same, full, 0.0).astype(BF16)


def forward_kernel(density_ref, out_ref, table_ref, buffer, sems):
    cas_square(table_ref)
    spec = lax.dot_general(table_ref[...], density_ref[...], (((1,), (1,)), ((), ())), preferred_element_type=F32)
    chunks = sems.shape[0]
    tiles = spec.shape[0] // 8 // chunks
    sent = []
    for c in range(chunks):
        part = spec[c * tiles * 8 : (c + 1) * tiles * 8]
        left = part[:, :LANES].reshape(tiles, 8, LANES)
        right = part[:, LANES:].reshape(tiles, 8, LANES)
        even, odd = swap_halves(left, right, 1)
        at = pl.ds(c * tiles, tiles)
        buffer[at, 0] = even.astype(BF16)
        buffer[at, 1] = odd.astype(BF16)
        sent.append(send(buffer.at[at], out_ref.at[at], sems.at[c]))
    for copy in sent:
        copy.wait()


def spectrum_kernel(moved_ref, table_ref, out_ref):
    pencils, groups = moved_ref.shape[:2]
    rows = groups * 8
    low, high = [], []
    for q in range(pencils // 2):
        left = moved_ref[2 * q].reshape(rows, LANES).astype(F32)
        right = moved_ref[2 * q + 1].reshape(rows, LANES).astype(F32)
        a, b = swap_halves(left, right, 1)
        low.append(a.astype(BF16))
        high.append(b.astype(BF16))
    data = jnp.concatenate([jnp.concatenate(low, axis=1), jnp.concatenate(high, axis=1)], axis=0)
    out_ref[...] = jnp.dot(data, table_ref[...], preferred_element_type=F32).astype(BF16)


def solve_kernel(spec_ref, forth_ref, back_ref, table_ref, *refs):
    *near_refs, keep_near_ref, keep_far_ref, came_near_ref, came_far_ref, out_ref = refs
    zspec = jnp.dot(forth_ref[...], spec_ref[...], preferred_element_type=F32)
    blocks = [ref[...] for ref in near_refs]
    for near_ref, far_ref in ((keep_near_ref, keep_far_ref), (came_near_ref, came_far_ref)):
        blocks.append(near_ref[0])
        blocks.extend(far_ref[i] for i in range(far_ref.shape[0]))
    parts, at = [], 0
    for block in blocks:
        parts.append((zspec[at : at + block.shape[0]] * block.astype(F32)).astype(BF16))
        at += block.shape[0]
    weighted = jnp.concatenate(parts, axis=0)
    total = jnp.dot(back_ref[...], weighted, preferred_element_type=F32).astype(BF16)
    values = jnp.dot(total, table_ref[...], preferred_element_type=F32)
    half = values.shape[0] // 2
    shape = out_ref.shape[1:]
    for q in range(out_ref.shape[0] // 2):
        at = slice(q * LANES, (q + 1) * LANES)
        a, b = swap_halves(values[:half, at], values[half:, at], 1)
        out_ref[2 * q] = a.astype(BF16).reshape(shape)
        out_ref[2 * q + 1] = b.astype(BF16).reshape(shape)


def inverse_kernel(came_ref, table_ref, out_ref, buffer, sems, *, scale):
    halves = swap_halves(came_ref[:, 0].astype(F32), came_ref[:, 1].astype(F32), 1)
    sent = []
    for i, half in enumerate(halves):
        data = half.reshape(half.shape[0] * 8, LANES).astype(BF16)
        out = lax.dot_general(data, table_ref[...], (((0,), (0,)), ((), ())), preferred_element_type=F32)
        at = pl.ds(i * LANES, LANES)
        buffer[at] = out * scale
        sent.append(send(buffer.at[at], out_ref.at[at], sems.at[i]))
    for copy in sent:
        copy.wait()


def along_z(z, s, steps, sign=1):
    return (z + sign * s) & (steps - 1)


def local(density, green):
    z_slab, x_local, y_cells = density.shape
    k_block, y_local, x_cells = green.shape
    groups = lax.axis_size("gz")
    pencils = lax.axis_size("pa")
    v_sub = y_local // groups
    z_freqs = k_block * groups
    lines = z_slab * x_local
    steps = groups // 2
    place = lax.axis_index("gz").astype(I32).reshape(1)

    near, far = (0, 1, steps - 1, 2, steps - 2), tuple(range(3, steps - 2))
    order = [(s, sy) for s in near[1:] for sy in (0, 1)] + [(s, sy) for sy in (0, 1) for s in (0, *far)]

    def shift_z(piece, s):
        pairs = [(i, along_z(i // 2, s, steps) * 2 + i % 2) for i in range(groups)]
        return lax.ppermute(piece, "gz", pairs)

    def swap_y(piece):
        return lax.ppermute(piece, "gz", [(i, i ^ 1) for i in range(groups)])

    rows = k_block * v_sub
    shared = array(len(near), rows, x_cells)
    keep_near, send_near, *outward = call(
        lambda *refs: split_kernel(*refs, near=near, far=far, steps=steps),
        (shared, shared) + (array(2 * rows, x_cells),) * len(far),
        place,
        green,
        specs=[SMEM, ANY],
        results=(VMEM, ANY) + (ANY,) * len(far),
        scratch_shapes=[
            pltpu.VMEM((steps, k_block, 2 * v_sub, x_cells), F32),
            pltpu.VMEM(shared.shape, BF16),
            pltpu.VMEM((len(far), 2 * rows, x_cells), BF16),
            pltpu.SemaphoreType.DMA((steps,)),
            pltpu.SemaphoreType.DMA((steps,)),
        ],
    )
    came_near = swap_y(send_near)
    inward = [shift_z(piece, s) for piece, s in zip(outward, far)]
    shared = array(len(far), rows, x_cells)
    keep_far, send_far = call(share_kernel, (pltpu.HBM(shared.shape, BF16),) * 2, place, *inward, specs=[SMEM] + [VMEM] * len(far))
    came_far = swap_y(send_far)
    pieces = call(join_kernel, (array(2 * rows, x_cells),) * (len(near) - 1), keep_near, came_near)
    pieces = [shift_z(piece, s) for piece, s in zip(pieces, near[1:])]

    forward, table = call(
        forward_kernel,
        (pltpu.HBM((y_cells // 8, 2, 8, LANES), BF16), array(y_cells, y_cells)),
        density.reshape(lines, y_cells),
        results=(ANY, VMEM),
        scratch_shapes=[pltpu.VMEM((y_cells // 8, 2, 8, LANES), BF16), pltpu.SemaphoreType.DMA((4,))],
    )
    moved = lax.all_to_all(
        forward.reshape(pencils * groups, 8, LANES), ("pa", "gz"), split_axis=0, concat_axis=0, tiled=True
    )
    spectrum = call(spectrum_kernel, array(groups * 16, x_cells), moved.reshape(pencils, groups, 8, LANES), table)
    forth, inverse_z = call(
        lambda *refs: expand_kernel(*refs, order=order, groups=groups, v_sub=v_sub, k_block=k_block, z_slab=z_slab),
        (pltpu.HBM((z_freqs * v_sub, groups * 16), BF16), pltpu.HBM((groups * 16, z_freqs * v_sub), BF16)),
        place,
        specs=[SMEM],
    )
    solved = call(
        solve_kernel,
        array(pencils, groups, 8, LANES),
        spectrum,
        forth,
        inverse_z,
        table,
        *pieces,
        keep_near,
        keep_far,
        came_near,
        came_far,
    )
    back = lax.all_to_all(
        solved.reshape(pencils * groups, 8, LANES), ("pa", "gz"), split_axis=0, concat_axis=0, tiled=True
    )
    scale = 1.0 / (x_cells * y_cells * z_freqs)
    out = call(
        lambda *refs: inverse_kernel(*refs, scale=scale),
        array(lines, y_cells, dtype=F32),
        back.reshape(y_cells // 8, 2, 8, LANES),
        table,
        results=ANY,
        scratch_shapes=[pltpu.VMEM((lines, y_cells), F32), pltpu.SemaphoreType.DMA((lines // LANES,))],
    )
    return out.reshape(z_slab, x_local, y_cells)


def solution(mesh):
    return jax.shard_map(
        local,
        mesh=mesh,
        in_specs=(P("gz", "pa", None), P("gz", "pa", None)),
        out_specs=P("gz", "pa", None),
        check_vma=False,
    )
```
